32 devices in a mesh: grp: 4 (over y, core), loc: 8 (over z, x).
Axes of the slice: x: 2, y: 2, z: 4, core: 2. Of those that a mesh axis runs over, the one named last changes fastest.
Arguments:
- tokens: bfloat16 [8192, 1024], P(('grp', 'loc')), may hold values from -6 to 6
- w_gate: bfloat16 [32, 1024, 2816], P(('grp', 'loc')), may hold values from -0.1875 to 0.1875
- w_up: bfloat16 [32, 1024, 2816], P(('grp', 'loc')), may hold values from -0.1875 to 0.1875
- w_down: bfloat16 [32, 2816, 1024], P(('grp', 'loc')), may hold values from -0.109375 to 0.109375
- chosen: int32 [32, 128], replicated, may hold values from -1 to 8191, as said below
- gate_weights: float32 [32, 128], replicated, may hold values from 0.05 to 1
Outputs:
- combined: bfloat16 [8192, 1024], P(('grp', 'loc'))
The draws below stay inside these ranges and needn't reach their ends.
Inputs may be any that keep to these rules, and one draw needn't show every extreme that they name: `chosen`: each entry is a token index or -1 for an empty slot, empty slots anywhere in a row. One expert's row names a token at most once. At most 8 entries of one expert's row lie among the 256 tokens of one device, and every expert has exactly 8 from some device. Some expert has no empty slot.
All inputs are finite; a program needn't handle non-finite values.
Results may differ from the reference program's by a relative error of at most 0.0085.
Values may be sent and summed in bfloat16 or wider, within the bound.
A program may use at most 128 MiB of HBM per device.

```python
import math
import jax
import jax.numpy as jnp
from jax import lax

D = 1024
FF = 2816
TOK_DEV = 256
PAIR_MOST = 8
EXPERTS = 32
CAP = 128
TOKENS = 8192


def draw_chosen(key, part):
    key_level, key_count, key_order, key_full, key_local, key_shuffle = jax.random.split(key, 6)
    load_level = jax.random.randint(key_level, (EXPERTS,), 0, 4)
    ceiling = jnp.minimum(jnp.array([5, 7, 9, 9], jnp.int32)[load_level], PAIR_MOST + 1)
    counts = jax.random.randint(key_count, (EXPERTS, EXPERTS), 0, ceiling[None, :])
    order_scores = jax.random.randint(key_order, (EXPERTS, EXPERTS), 0, 1 << 18) * EXPERTS + jnp.arange(EXPERTS)[None, :]
    source_order = jnp.argsort(order_scores, axis=1).astype(jnp.int32)
    ordered = jnp.take_along_axis(counts, source_order, axis=1)
    full_expert = jax.random.randint(key_full, (), 0, EXPERTS)
    row_iota = jnp.arange(EXPERTS)[:, None]
    column_iota = jnp.arange(EXPERTS)[None, :]
    ordered = jnp.where((column_iota == 0) | (row_iota == full_expert), PAIR_MOST, ordered)
    before = jnp.cumsum(ordered, axis=1) - ordered
    kept_count = jnp.minimum(jnp.maximum(CAP - before, 0), ordered)
    scores = jax.random.randint(key_local, (EXPERTS, EXPERTS, TOK_DEV), 0, 1 << 18) * TOK_DEV + jnp.arange(TOK_DEV)[None, None, :]
    local_pick = jnp.argsort(scores, axis=2)[:, :, :PAIR_MOST].astype(jnp.int32)
    global_id = source_order[:, :, None] * TOK_DEV + local_pick
    pair_iota = jnp.arange(PAIR_MOST)[None, None, :]
    is_valid = pair_iota < kept_count[:, :, None]
    slot_index = jnp.where(is_valid, before[:, :, None] + pair_iota, CAP)
    expert_ids = jnp.broadcast_to(row_iota[:, :, None], slot_index.shape)
    slot_table = jnp.full((EXPERTS, CAP), -1, jnp.int32).at[expert_ids, slot_index].set(global_id.astype(jnp.int32), mode='drop')
    shuffle_scores = jax.random.randint(key_shuffle, (EXPERTS, CAP), 0, 1 << 18) * CAP + jnp.arange(CAP)[None, :]
    shuffle = jnp.argsort(shuffle_scores, axis=1)
    return jnp.take_along_axis(slot_table, shuffle, axis=1)


def block_scale(key, dims, pieces, least, top_value):
    def one(axis_at, blocks):
        steps = jax.random.uniform(jax.random.fold_in(jax.random.fold_in(key, 6), axis_at), (blocks,), jnp.float32, least / len(pieces), top_value / len(pieces))
        return jnp.repeat(jnp.exp(steps), dims[axis_at] // blocks).reshape((-1,) + (1,) * (len(dims) - axis_at - 1))

    loudness = one(*pieces[0])
    for cut in pieces[1:]:
        loudness = loudness * one(*cut)
    return loudness


def centred(stream_key, dims, scale, most, cuts=(), kind=jnp.bfloat16):
    gain = block_scale(stream_key, dims, cuts, -0.22, 0.18) if cuts else 1.0
    drawn = jax.random.normal(stream_key, dims, jnp.float32) * scale * gain
    return jnp.minimum(jnp.maximum(drawn, -most), most).astype(kind)


def setup_inputs(seed: int = 0) -> dict:
    splits = jax.random.split(jax.random.key(seed), 7)
    return {
        "tokens": centred(splits[0], (TOKENS, D), 1.0, 6.0, ((0, 32),)),
        "w_gate": centred(splits[1], (EXPERTS, D, FF), D ** -0.5, 0.1875, ((0, 32),)),
        "w_up": centred(splits[2], (EXPERTS, D, FF), D ** -0.5, 0.1875, ((0, 32),)),
        "w_down": centred(splits[3], (EXPERTS, FF, D), FF ** -0.5, 0.109375, ((0, 32),)),
        "chosen": draw_chosen(jax.random.fold_in(splits[6], 71), 0),
        "gate_weights": jnp.clip(jnp.exp(jax.random.uniform(splits[5], (EXPERTS, CAP), jnp.float32, math.log(0.05), math.log(1.0))), 0.05, 1.0),
    }


def reference(tokens, w_gate, w_up, w_down, chosen, gate_weights):
    token_total = tokens.shape[0]
    model_width = tokens.shape[1]
    padded = jnp.concatenate([tokens, jnp.zeros((1, model_width), tokens.dtype)], axis=0)

    def one_expert(expert, running):
        picks = lax.dynamic_index_in_dim(chosen, expert, 0, keepdims=False)
        is_live = picks >= 0
        row_index = jnp.where(is_live, picks, token_total).astype(jnp.int32)
        row_block = jnp.take(padded, row_index, axis=0)
        gate_mat = lax.dynamic_index_in_dim(w_gate, expert, 0, keepdims=False)
        up_mat = lax.dynamic_index_in_dim(w_up, expert, 0, keepdims=False)
        down_mat = lax.dynamic_index_in_dim(w_down, expert, 0, keepdims=False)
        gate_pre = jnp.dot(row_block, gate_mat, preferred_element_type=jnp.float32)
        up_pre = jnp.dot(row_block, up_mat, preferred_element_type=jnp.float32)
        hidden = (jax.nn.silu(gate_pre) * up_pre).astype(jnp.bfloat16)
        expert_out = jnp.dot(hidden, down_mat, preferred_element_type=jnp.float32).astype(jnp.bfloat16)
        slot_weight = jnp.where(is_live, lax.dynamic_index_in_dim(gate_weights, expert, 0, keepdims=False), 0.0)
        weighted = slot_weight[:, None] * expert_out.astype(jnp.float32)
        return running.at[row_index].add(weighted)

    running = jnp.zeros((token_total + 1, model_width), jnp.float32)
    running = lax.fori_loop(0, EXPERTS, one_expert, running)
    return running[:token_total].astype(jnp.bfloat16)
```

```python
import functools

import jax
import jax.numpy as jnp
from jax import lax
from jax.experimental import pallas as pl
from jax.experimental.pallas import tpu as pltpu
from jax.sharding import PartitionSpec as P

PAIR_MOST = 8
WIDE = 256
WEIGHT_CUTS = 4
MESH = pl.DeviceIdType.MESH
F32 = jnp.float32
BF16 = jnp.bfloat16


def plan(local_count):
    half = local_count // 2
    far_even = [(1, j) for j in range(0, half, 2)]
    far_odd = [(1, j) for j in range(1, half, 2)]
    near = [(0, j) for j in range(half)]
    if half % 2:
        return [far_even + far_odd + near]
    return [far_even + near, far_odd]


def tile_of(size):
    for tile in (WIDE, 128):
        if size % tile == 0:
            return tile
    return size


def kernel(
    passes,
    tokens_hbm,
    gate_hbm,
    up_hbm,
    down_hbm,
    chosen_hbm,
    weight_hbm,
    out_ref,
    tokens,
    w_gate,
    w_up,
    w_down,
    chosen,
    weights,
    chosen_rows,
    weight_rows,
    outgoing,
    received,
    produced,
    back,
    gathered,
    hidden,
    total,
    *rest,
):
    mix_hi, mix_lo = rest[: len(passes)], rest[len(passes) : 2 * len(passes)]
    small_sem, load_sem, send_sem, recv_sem, return_send_sem, return_sem = rest[2 * len(passes) :]
    group_count, local_count = lax.axis_size("grp"), lax.axis_size("loc")
    devices = group_count * local_count
    half = local_count // 2
    grp, loc = lax.axis_index("grp"), lax.axis_index("loc")
    me = grp * local_count + loc
    side, spot = loc // half, loc % half
    groups = [group for one in passes for group in one]

    blocks = []
    starts = [0]
    for number, one in enumerate(passes):
        for flip, step in one:
            for turn in range(group_count):
                peer_grp = lax.rem(grp + turn, group_count)
                peer_loc = lax.rem(side + flip, 2) * half + lax.rem(spot + step, half)
                mirror = groups.index((flip, (half - step) % half)) * group_count
                mirror += (group_count - turn) % group_count
                own = flip == 0 and step == 0 and turn == 0
                blocks.append((number, peer_grp, peer_loc, mirror, own))
        starts.append(len(blocks))

    barrier = pltpu.get_barrier_semaphore()

    def greet(turn, carry):
        peer = lax.rem(me + turn, devices)
        pl.semaphore_signal(
            barrier, inc=1, device_id=(peer // local_count, peer % local_count), device_id_type=MESH
        )
        return carry

    lax.fori_loop(1, devices, greet, 0)

    small = [
        pltpu.make_async_copy(chosen_hbm, chosen, small_sem.at[0]),
        pltpu.make_async_copy(weight_hbm, weights, small_sem.at[1]),
        pltpu.make_async_copy(tokens_hbm, tokens, small_sem.at[2]),
    ]
    for copy in small:
        copy.start()
    small[0].wait()
    small[1].wait()
    slot_total = chosen.shape[1]
    for at, (_, peer_grp, peer_loc, _, _) in enumerate(blocks):
        expert = peer_grp * local_count + peer_loc
        rows = pl.ds(at * PAIR_MOST, PAIR_MOST)
        chosen_rows[rows, :] = jnp.broadcast_to(
            chosen[pl.ds(expert, 1), :], (PAIR_MOST, slot_total)
        )
        weight_rows[rows, :] = jnp.broadcast_to(
            weights[pl.ds(expert, 1), :], (PAIR_MOST, slot_total)
        )
    token_count, width = tokens.shape
    row_total = devices * PAIR_MOST
    local = chosen_rows[...] - me * token_count
    mine = (local >= 0) & (local < token_count)
    earlier = lax.broadcasted_iota(jnp.int32, (slot_total, slot_total), 0)
    later = lax.broadcasted_iota(jnp.int32, (slot_total, slot_total), 1)
    before = jnp.where(earlier < later, 1.0, 0.0).astype(BF16)
    rank = jnp.dot(
        jnp.where(mine, 1.0, 0.0).astype(BF16), before, preferred_element_type=F32
    )
    wanted = lax.broadcasted_iota(jnp.int32, (row_total, slot_total), 0) % PAIR_MOST
    hit = mine & (rank == wanted.astype(F32))
    pick = jnp.sum(jnp.where(hit, local.astype(F32) + 1.0, 0.0), axis=1, keepdims=True) - 1.0
    pick_weight = jnp.sum(jnp.where(hit, weight_rows[...], 0.0), axis=1, keepdims=True)
    token_iota = lax.broadcasted_iota(jnp.int32, (row_total, token_count), 1).astype(F32)
    select = pick == token_iota
    select_table = jnp.where(select, 1.0, 0.0).astype(BF16)
    small[2].wait()
    loads = []
    for number, (source, place) in enumerate(
        ((gate_hbm, w_gate), (up_hbm, w_up), (down_hbm, w_down))
    ):
        depth = place.shape[0] // WEIGHT_CUTS
        for cut in range(WEIGHT_CUTS):
            rows = pl.ds(cut * depth, depth)
            copy = pltpu.make_async_copy(
                source.at[0, rows], place.at[rows], load_sem.at[number * WEIGHT_CUTS + cut]
            )
            copy.start()
            loads.append(copy)

    picked = jnp.dot(select_table, tokens[...], preferred_element_type=F32)
    outgoing[...] = picked.reshape(devices, PAIR_MOST, width).astype(BF16)

    pl.semaphore_wait(barrier, devices - 1)

    def send(source, place, send_sems, recv_sems, at):
        number, peer_grp, peer_loc, mirror, own = blocks[at]
        if own:
            pltpu.make_async_copy(source.at[at], place.at[mirror], recv_sems.at[number]).start()
        else:
            pltpu.make_async_remote_copy(
                src_ref=source.at[at],
                dst_ref=place.at[mirror],
                send_sem=send_sems.at[0],
                recv_sem=recv_sems.at[number],
                device_id=(peer_grp, peer_loc),
                device_id_type=MESH,
            ).start()

    def wait_blocks(place, sem, first, count):
        view = place.at[pl.ds(first, count)]
        pltpu.make_async_copy(view, view, sem).wait()

    for at in range(devices):
        send(outgoing, received, send_sem, recv_sem, at)

    mixing = jnp.where(select, pick_weight, 0.0)
    for number in range(len(passes)):
        first, last = starts[number] * PAIR_MOST, starts[number + 1] * PAIR_MOST
        turned = mixing[first:last].T
        high = turned.astype(BF16)
        mix_hi[number][...] = high
        mix_lo[number][...] = (turned - high.astype(F32)).astype(BF16)

    for copy in loads:
        copy.wait()

    hidden_total = w_gate.shape[1]
    hidden_tile, width_tile = tile_of(hidden_total), tile_of(width)
    for number in range(len(passes)):
        first, count = starts[number], starts[number + 1] - starts[number]
        rows = count * PAIR_MOST
        wait_blocks(received, recv_sem.at[number], first, count)
        arrived = received[pl.ds(first, count)].astype(F32)
        gathered[:rows, :] = arrived.reshape(rows, width).astype(BF16)

        def expand(tile, carry, rows=rows):
            columns = pl.ds(pl.multiple_of(tile * hidden_tile, hidden_tile), hidden_tile)
            gate_pre = jnp.dot(gathered[:rows, :], w_gate[:, columns], preferred_element_type=F32)
            up_pre = jnp.dot(gathered[:rows, :], w_up[:, columns], preferred_element_type=F32)
            hidden[:rows, columns] = (gate_pre / (1.0 + jnp.exp(-gate_pre)) * up_pre).astype(BF16)
            return carry

        lax.fori_loop(0, hidden_total // hidden_tile, expand, 0, unroll=True)

        def contract(tile, carry, rows=rows, first=first, count=count):
            columns = pl.ds(pl.multiple_of(tile * width_tile, width_tile), width_tile)
            result = jnp.dot(hidden[:rows, :], w_down[:, columns], preferred_element_type=F32)
            produced[pl.ds(first, count), :, columns] = result.reshape(
                count, PAIR_MOST, width_tile
            ).astype(BF16)
            return carry

        lax.fori_loop(0, width // width_tile, contract, 0, unroll=True)
        for at in range(first, first + count):
            send(produced, back, return_send_sem, return_sem, at)

    for number in range(len(passes)):
        first, count = starts[number], starts[number + 1] - starts[number]
        rows = count * PAIR_MOST
        wait_blocks(back, return_sem.at[number], first, count)
        returned = back[pl.ds(first, count)].astype(F32).reshape(rows, width).astype(BF16)
        part = jnp.dot(mix_hi[number][...], returned, preferred_element_type=F32)
        part += jnp.dot(mix_lo[number][...], returned, preferred_element_type=F32)
        if number:
            part += total[...]
        if number == len(passes) - 1:
            out_ref[...] = part.astype(out_ref.dtype)
        else:
            total[...] = part
    wait_blocks(outgoing, send_sem.at[0], 0, devices - 1)
    wait_blocks(produced, return_send_sem.at[0], 0, devices - 1)


def shards(tokens, w_gate, w_up, w_down, chosen, gate_weights):
    local_count = lax.axis_size("loc")
    devices = lax.axis_size("grp") * local_count
    passes = plan(local_count)
    token_count, width = tokens.shape
    hidden_total = w_gate.shape[2]
    row_total = devices * PAIR_MOST
    pass_rows = [len(one) * lax.axis_size("grp") * PAIR_MOST for one in passes]
    table = pltpu.VMEM((devices, PAIR_MOST, width), BF16)
    anywhere = pl.BlockSpec(memory_space=pl.ANY)
    return pl.pallas_call(
        functools.partial(kernel, passes),
        out_shape=pltpu.VMEM((token_count, width), BF16),
        in_specs=[anywhere] * 6,
        out_specs=pl.BlockSpec(memory_space=pltpu.VMEM),
        scratch_shapes=[
            pltpu.VMEM((token_count, width), BF16),
            pltpu.VMEM(w_gate.shape[1:], BF16),
            pltpu.VMEM(w_up.shape[1:], BF16),
            pltpu.VMEM(w_down.shape[1:], BF16),
            pltpu.VMEM(chosen.shape, jnp.int32),
            pltpu.VMEM(chosen.shape, F32),
            pltpu.VMEM((row_total, chosen.shape[1]), jnp.int32),
            pltpu.VMEM((row_total, chosen.shape[1]), F32),
            table,
            table,
            table,
            table,
            pltpu.VMEM((max(pass_rows), width), BF16),
            pltpu.VMEM((max(pass_rows), hidden_total), BF16),
            pltpu.VMEM((token_count, width), F32),
            *[pltpu.VMEM((token_count, rows), BF16) for rows in pass_rows],
            *[pltpu.VMEM((token_count, rows), BF16) for rows in pass_rows],
            pltpu.SemaphoreType.DMA((3,)),
            pltpu.SemaphoreType.DMA((3 * WEIGHT_CUTS,)),
            pltpu.SemaphoreType.DMA((1,)),
            pltpu.SemaphoreType.DMA((len(passes),)),
            pltpu.SemaphoreType.DMA((1,)),
            pltpu.SemaphoreType.DMA((len(passes),)),
        ],
        compiler_params=pltpu.CompilerParams(
            collective_id=0, has_side_effects=True, vmem_limit_bytes=58 * 1024 * 1024
        ),
    )(tokens, w_gate, w_up, w_down, chosen, gate_weights)


def solution(mesh):
    return jax.shard_map(
        shards,
        mesh=mesh,
        in_specs=(
            P(("grp", "loc"), None),
            P(("grp", "loc"), None, None),
            P(("grp", "loc"), None, None),
            P(("grp", "loc"), None, None),
            P(),
            P(),
        ),
        out_specs=P(("grp", "loc"), None),
        check_vma=False,
    )
```

```python
import jax
import jax.numpy as jnp
from jax import lax
from jax.experimental import pallas as pl
from jax.experimental.pallas import tpu as pltpu
from jax.sharding import PartitionSpec as P

PAIR_MOST = 8
WIDE = 256
WEIGHT_CUTS = 4
MESH = pl.DeviceIdType.MESH
F32 = jnp.float32
BF16 = jnp.bfloat16


def tile_of(size):
    for tile in (WIDE, 128):
        if size % tile == 0:
            return tile
    return size


def flip(value, mask):
    bit = 1
    while bit <= mask:
        if mask & bit:
            value = value + bit - 2 * bit * (value // bit % 2)
        bit *= 2
    return value


def kernel(
    tokens_hbm,
    gate_hbm,
    up_hbm,
    down_hbm,
    chosen_hbm,
    weight_hbm,
    out_ref,
    tokens,
    w_gate,
    w_up,
    w_down,
    chosen,
    weights,
    chosen_rows,
    weight_rows,
    outgoing,
    received,
    produced,
    back,
    gathered,
    hidden,
    total,
    mix_hi,
    mix_lo,
    small_sem,
    load_sem,
    send_sem,
    recv_sem,
    return_send_sem,
    return_sem,
):
    group_count, local_count = lax.axis_size("grp"), lax.axis_size("loc")
    devices = group_count * local_count
    quarter = local_count // 4
    grp, loc = lax.axis_index("grp"), lax.axis_index("loc")
    me = grp * local_count + loc
    plane, spot = loc // quarter, loc % quarter
    side = plane // 2
    outer = (side + plane % 2 + 1) % 2
    block = quarter * group_count
    part = block // 2

    def partner(plane_there, turn):
        return (
            flip(grp, turn % group_count),
            plane_there * quarter + flip(spot, turn // group_count),
        )

    def far_plane(kind):
        return side * (1 - kind) + (1 - side) * (2 + kind)

    def near_out(other, turn):
        return other * block + turn

    def far_out(sub, kind, turn):
        return (2 + sub) * block + kind * part + turn

    def near_in(other, turn):
        return other * (block + part) + turn

    def far_in(sub, kind, turn):
        return turn + (7 * part - kind * part if sub else block + kind * (block + part))

    def far_pass(sub, kind):
        return 3 - kind if sub else kind

    dispatch, results = [], [[], [], [], []]
    for sub in range(2):
        for turn in range(part):
            for kind in range(2):
                peer = partner(far_plane(kind), sub * part + turn)
                there, number = far_in(sub, outer, turn), far_pass(sub, outer)
                dispatch.append((far_out(sub, kind, turn), peer, there, number))
                home = far_out(sub, outer, turn)
                results[far_pass(sub, kind)].append((far_in(sub, kind, turn), peer, home, 1 + sub))
    near = []
    for other in (1, 0):
        for turn in range(block):
            peer = partner(flip(plane, other), turn)
            near.append((near_out(other, turn), peer, near_in(other, turn), other))
            results[other].append((near_in(other, turn), peer, near_out(other, turn), 0))
    dispatch = near + dispatch
    passes = [
        (0, block + part), (block + part, block + part), (6 * part, part), (7 * part, part)
    ]
    groups = [(0, 2 * block), (2 * block, block), (3 * block, block)]
    barrier = pltpu.get_barrier_semaphore()
    for at, peer, _, _ in reversed(dispatch):
        if at:
            pl.semaphore_signal(barrier, inc=1, device_id=peer, device_id_type=MESH)
    small = [
        pltpu.make_async_copy(chosen_hbm, chosen, small_sem.at[0]),
        pltpu.make_async_copy(weight_hbm, weights, small_sem.at[1]),
        pltpu.make_async_copy(tokens_hbm, tokens, small_sem.at[2]),
    ]
    for copy in small:
        copy.start()

    small[0].wait()
    small[1].wait()
    slot_total = chosen.shape[1]
    for at, (peer_grp, peer_loc), _, _ in dispatch:
        expert = peer_grp * local_count + peer_loc
        rows = pl.ds(at * PAIR_MOST, PAIR_MOST)
        chosen_rows[rows, :] = jnp.broadcast_to(
            chosen[pl.ds(expert, 1), :], (PAIR_MOST, slot_total)
        )
        weight_rows[rows, :] = jnp.broadcast_to(
            weights[pl.ds(expert, 1), :], (PAIR_MOST, slot_total)
        )
    token_count, width = tokens.shape
    row_total = devices * PAIR_MOST
    local = chosen_rows[...] - me * token_count
    mine = (local >= 0) & (local < token_count)
    earlier = lax.broadcasted_iota(jnp.int32, (slot_total, slot_total), 0)
    later = lax.broadcasted_iota(jnp.int32, (slot_total, slot_total), 1)
    before = jnp.where(earlier < later, 1.0, 0.0).astype(BF16)
    rank = jnp.dot(
        jnp.where(mine, 1.0, 0.0).astype(BF16), before, preferred_element_type=F32
    )
    wanted = lax.broadcasted_iota(jnp.int32, (row_total, slot_total), 0) % PAIR_MOST
    hit = mine & (rank == wanted.astype(F32))
    pick = jnp.sum(jnp.where(hit, local.astype(F32) + 1.0, 0.0), axis=1, keepdims=True) - 1.0
    pick_weight = jnp.sum(jnp.where(hit, weight_rows[...], 0.0), axis=1, keepdims=True)
    token_iota = lax.broadcasted_iota(jnp.int32, (row_total, token_count), 1).astype(F32)
    select = pick == token_iota
    select_table = jnp.where(select, 1.0, 0.0).astype(BF16)
    small[2].wait()
    loads = []
    for number, (source, place) in enumerate(
        ((gate_hbm, w_gate), (up_hbm, w_up), (down_hbm, w_down))
    ):
        depth = place.shape[0] // WEIGHT_CUTS
        for cut in range(WEIGHT_CUTS):
            rows = pl.ds(cut * depth, depth)
            copy = pltpu.make_async_copy(
                source.at[0, rows], place.at[rows], load_sem.at[number * WEIGHT_CUTS + cut]
            )
            copy.start()
            loads.append(copy)
    picked = jnp.dot(select_table, tokens[...], preferred_element_type=F32)
    outgoing[...] = picked.reshape(devices, PAIR_MOST, width).astype(BF16)
    pl.semaphore_wait(barrier, devices - 1)

    def send(source, place, send_sems, sems, entry):
        at, peer, mirror, sem = entry
        if at:
            pltpu.make_async_remote_copy(
                src_ref=source.at[at],
                dst_ref=place.at[mirror],
                send_sem=send_sems.at[0],
                recv_sem=sems.at[sem],
                device_id=peer,
                device_id_type=MESH,
            ).start()
        else:
            pltpu.make_async_copy(source.at[at], place.at[mirror], sems.at[sem]).start()

    def wait_blocks(place, sem, first, count):
        view = place.at[pl.ds(first, count)]
        pltpu.make_async_copy(view, view, sem).wait()

    for entry in dispatch:
        send(outgoing, received, send_sem, recv_sem, entry)
    mixing = jnp.where(select, pick_weight, 0.0).T
    high = mixing.astype(BF16)
    low = (mixing - high.astype(F32)).astype(BF16)
    for number, (first, count) in enumerate(groups):
        rows = slice(first * PAIR_MOST, (first + count) * PAIR_MOST)
        mix_hi[number][...] = high[:, rows]
        mix_lo[number][...] = low[:, rows]
    for copy in loads:
        copy.wait()

    hidden_total = w_gate.shape[1]
    hidden_tile, width_tile = tile_of(hidden_total), tile_of(width)
    for number, (first, count) in enumerate(passes):
        rows = count * PAIR_MOST
        wait_blocks(received, recv_sem.at[number], first, count)
        arrived = received[pl.ds(first, count)].astype(F32)
        gathered[:rows, :] = arrived.reshape(rows, width).astype(BF16)

        def expand(tile, carry, rows=rows):
            columns = pl.ds(pl.multiple_of(tile * hidden_tile, hidden_tile), hidden_tile)
            gate_pre = jnp.dot(gathered[:rows, :], w_gate[:, columns], preferred_element_type=F32)
            up_pre = jnp.dot(gathered[:rows, :], w_up[:, columns], preferred_element_type=F32)
            hidden[:rows, columns] = (gate_pre / (1.0 + jnp.exp(-gate_pre)) * up_pre).astype(BF16)
            return carry

        lax.fori_loop(0, hidden_total // hidden_tile, expand, 0, unroll=True)

        def contract(tile, carry, rows=rows, first=first, count=count):
            columns = pl.ds(pl.multiple_of(tile * width_tile, width_tile), width_tile)
            result = jnp.dot(hidden[:rows, :], w_down[:, columns], preferred_element_type=F32)
            produced[pl.ds(first, count), :, columns] = result.reshape(
                count, PAIR_MOST, width_tile
            ).astype(BF16)
            return carry

        lax.fori_loop(0, width // width_tile, contract, 0, unroll=True)
        for entry in results[number]:
            send(produced, back, return_send_sem, return_sem, entry)

    for number, (first, count) in enumerate(groups):
        rows = count * PAIR_MOST
        wait_blocks(back, return_sem.at[number], first, count)
        returned = back[pl.ds(first, count)].astype(F32).reshape(rows, width).astype(BF16)
        result = jnp.dot(mix_hi[number][...], returned, preferred_element_type=F32)
        result += jnp.dot(mix_lo[number][...], returned, preferred_element_type=F32)
        if number:
            result += total[...]
        if number == len(groups) - 1:
            out_ref[...] = result.astype(out_ref.dtype)
        else:
            total[...] = result
    wait_blocks(outgoing, send_sem.at[0], 0, devices - 1)
    wait_blocks(produced, return_send_sem.at[0], 0, devices - 1)


def shards(tokens, w_gate, w_up, w_down, chosen, gate_weights):
    local_count = lax.axis_size("loc")
    devices = lax.axis_size("grp") * local_count
    token_count, width = tokens.shape
    hidden_total = w_gate.shape[2]
    row_total = devices * PAIR_MOST
    pass_rows = row_total * 3 // 8
    group_rows = [row_total // 2, row_total // 4, row_total // 4]
    table = pltpu.VMEM((devices, PAIR_MOST, width), BF16)
    mixes = [pltpu.VMEM((token_count, rows), BF16) for rows in group_rows]
    anywhere = pl.BlockSpec(memory_space=pl.ANY)
    return pl.pallas_call(
        kernel,
        out_shape=pltpu.VMEM((token_count, width), BF16),
        in_specs=[anywhere] * 6,
        out_specs=pl.BlockSpec(memory_space=pltpu.VMEM),
        scratch_shapes=[
            pltpu.VMEM((token_count, width), BF16),
            pltpu.VMEM(w_gate.shape[1:], BF16),
            pltpu.VMEM(w_up.shape[1:], BF16),
            pltpu.VMEM(w_down.shape[1:], BF16),
            pltpu.VMEM(chosen.shape, jnp.int32),
            pltpu.VMEM(chosen.shape, F32),
            pltpu.VMEM((row_total, chosen.shape[1]), jnp.int32),
            pltpu.VMEM((row_total, chosen.shape[1]), F32),
            table,
            table,
            table,
            table,
            pltpu.VMEM((pass_rows, width), BF16),
            pltpu.VMEM((pass_rows, hidden_total), BF16),
            pltpu.VMEM((token_count, width), F32),
            mixes,
            mixes,
            pltpu.SemaphoreType.DMA((3,)),
            pltpu.SemaphoreType.DMA((3 * WEIGHT_CUTS,)),
            pltpu.SemaphoreType.DMA((1,)),
            pltpu.SemaphoreType.DMA((4,)),
            pltpu.SemaphoreType.DMA((1,)),
            pltpu.SemaphoreType.DMA((3,)),
        ],
        compiler_params=pltpu.CompilerParams(
            collective_id=0, has_side_effects=True, vmem_limit_bytes=58 * 1024 * 1024
        ),
    )(tokens, w_gate, w_up, w_down, chosen, gate_weights)


def solution(mesh):
    return jax.shard_map(
        shards,
        mesh=mesh,
        in_specs=(
            P(("grp", "loc"), None),
            P(("grp", "loc"), None, None),
            P(("grp", "loc"), None, None),
            P(("grp", "loc"), None, None),
            P(),
            P(),
        ),
        out_specs=P(("grp", "loc"), None),
        check_vma=False,
    )
```

```python
import jax
import jax.numpy as jnp
from jax import lax
from jax.experimental import pallas as pl
from jax.experimental.pallas import tpu as pltpu
from jax.sharding import PartitionSpec as P

PAIR_MOST = 8
WIDE = 256
WEIGHT_CUTS = 4
MESH = pl.DeviceIdType.MESH
F32 = jnp.float32
BF16 = jnp.bfloat16


def tile_of(size):
    for tile in (WIDE, 128):
        if size % tile == 0:
            return tile
    return size


def cuts(block):
    early = block * 3 // 8
    return early, block - early


def group_sizes(block):
    early, late = cuts(block)
    return [2 * block, 2 * early, 2 * late]


def flip(value, mask):
    bit = 1
    while bit <= mask:
        if mask & bit:
            value = value + bit - 2 * bit * (value // bit % 2)
        bit *= 2
    return value


def kernel(
    tokens_hbm,
    gate_hbm,
    up_hbm,
    down_hbm,
    chosen_hbm,
    weight_hbm,
    out_ref,
    tokens,
    w_gate,
    w_up,
    w_down,
    chosen,
    weights,
    chosen_rows,
    weight_rows,
    outgoing,
    received,
    produced,
    back,
    gathered,
    hidden,
    total,
    mix_hi,
    mix_lo,
    small_sem,
    load_sem,
    send_sem,
    recv_sem,
    return_send_sem,
    return_sem,
):
    group_count, local_count = lax.axis_size("grp"), lax.axis_size("loc")
    devices = group_count * local_count
    quarter = local_count // 4
    grp, loc = lax.axis_index("grp"), lax.axis_index("loc")
    me = grp * local_count + loc
    plane, spot = loc // quarter, loc % quarter
    side = plane // 2
    outer = (side + plane % 2 + 1) % 2
    block = quarter * group_count
    early, late = cuts(block)

    def partner(plane_there, turn):
        return (
            flip(grp, turn % group_count),
            plane_there * quarter + flip(spot, turn // group_count),
        )

    def far_plane(kind):
        return side * (1 - kind) + (1 - side) * (2 + kind)

    def near_out(other, turn):
        return other * block + turn

    def far_out(sub, kind, turn):
        if sub:
            return 2 * block + 2 * early + kind * late + turn
        return 2 * block + kind * early + turn

    def near_in(other, turn):
        return other * (block + early) + turn

    def far_in(sub, kind, turn):
        if sub:
            return 2 * (block + early) + (1 - kind) * late + turn
        return block + kind * (block + early) + turn

    def far_pass(sub, kind):
        return 3 - kind if sub else kind

    dispatch, results = [], [[], [], [], []]
    for sub, count in enumerate((early, late)):
        for turn in range(count):
            for kind in range(2):
                peer = partner(far_plane(kind), sub * early + turn)
                there, number = far_in(sub, outer, turn), far_pass(sub, outer)
                dispatch.append((far_out(sub, kind, turn), peer, there, number))
                home = far_out(sub, outer, turn)
                results[far_pass(sub, kind)].append((far_in(sub, kind, turn), peer, home, 1 + sub))
    near = []
    for other in (1, 0):
        for turn in range(block):
            peer = partner(flip(plane, other), turn)
            near.append((near_out(other, turn), peer, near_in(other, turn), other))
            results[other].append((near_in(other, turn), peer, near_out(other, turn), 0))
    dispatch = near + dispatch
    counts = [block + early, block + early, late, late]
    passes = [(sum(counts[:number]), count) for number, count in enumerate(counts)]
    counts = group_sizes(block)
    groups = [(sum(counts[:number]), count) for number, count in enumerate(counts)]
    barrier = pltpu.get_barrier_semaphore()
    for at, peer, _, _ in reversed(dispatch):
        if at:
            pl.semaphore_signal(barrier, inc=1, device_id=peer, device_id_type=MESH)
    small = [
        pltpu.make_async_copy(chosen_hbm, chosen, small_sem.at[0]),
        pltpu.make_async_copy(weight_hbm, weights, small_sem.at[1]),
        pltpu.make_async_copy(tokens_hbm, tokens, small_sem.at[2]),
    ]
    for copy in small:
        copy.start()

    small[0].wait()
    small[1].wait()
    slot_total = chosen.shape[1]
    for at, (peer_grp, peer_loc), _, _ in dispatch:
        expert = peer_grp * local_count + peer_loc
        rows = pl.ds(at * PAIR_MOST, PAIR_MOST)
        chosen_rows[rows, :] = jnp.broadcast_to(
            chosen[pl.ds(expert, 1), :], (PAIR_MOST, slot_total)
        )
        weight_rows[rows, :] = jnp.broadcast_to(
            weights[pl.ds(expert, 1), :], (PAIR_MOST, slot_total)
        )
    token_count, width = tokens.shape
    row_total = devices * PAIR_MOST
    local = chosen_rows[...] - me * token_count
    mine = (local >= 0) & (local < token_count)
    earlier = lax.broadcasted_iota(jnp.int32, (slot_total, slot_total), 0)
    later = lax.broadcasted_iota(jnp.int32, (slot_total, slot_total), 1)
    before = jnp.where(earlier < later, 1.0, 0.0).astype(BF16)
    rank = jnp.dot(
        jnp.where(mine, 1.0, 0.0).astype(BF16), before, preferred_element_type=F32
    )
    wanted = lax.broadcasted_iota(jnp.int32, (row_total, slot_total), 0) % PAIR_MOST
    hit = mine & (rank == wanted.astype(F32))
    pick = jnp.sum(jnp.where(hit, local.astype(F32) + 1.0, 0.0), axis=1, keepdims=True) - 1.0
    pick_weight = jnp.sum(jnp.where(hit, weight_rows[...], 0.0), axis=1, keepdims=True)
    token_iota = lax.broadcasted_iota(jnp.int32, (row_total, token_count), 1).astype(F32)
    select = pick == token_iota
    select_table = jnp.where(select, 1.0, 0.0).astype(BF16)
    small[2].wait()
    loads = []
    for number, (source, place) in enumerate(
        ((gate_hbm, w_gate), (up_hbm, w_up), (down_hbm, w_down))
    ):
        depth = place.shape[0] // WEIGHT_CUTS
        for cut in range(WEIGHT_CUTS):
            rows = pl.ds(cut * depth, depth)
            copy = pltpu.make_async_copy(
                source.at[0, rows], place.at[rows], load_sem.at[number * WEIGHT_CUTS + cut]
            )
            copy.start()
            loads.append(copy)
    picked = jnp.dot(select_table, tokens[...], preferred_element_type=F32)
    outgoing[...] = picked.reshape(devices, PAIR_MOST, width).astype(BF16)
    pl.semaphore_wait(barrier, devices - 1)

    def send(source, place, send_sems, sems, entry):
        at, peer, mirror, sem = entry
        if at:
            pltpu.make_async_remote_copy(
                src_ref=source.at[at],
                dst_ref=place.at[mirror],
                send_sem=send_sems.at[0],
                recv_sem=sems.at[sem],
                device_id=peer,
                device_id_type=MESH,
            ).start()
        else:
            pltpu.make_async_copy(source.at[at], place.at[mirror], sems.at[sem]).start()

    def wait_blocks(place, sem, first, count):
        view = place.at[pl.ds(first, count)]
        pltpu.make_async_copy(view, view, sem).wait()

    for entry in dispatch:
        send(outgoing, received, send_sem, recv_sem, entry)
    mixing = jnp.where(select, pick_weight, 0.0).T
    high = mixing.astype(BF16)
    low = (mixing - high.astype(F32)).astype(BF16)
    for number, (first, count) in enumerate(groups):
        rows = slice(first * PAIR_MOST, (first + count) * PAIR_MOST)
        mix_hi[number][...] = high[:, rows]
        mix_lo[number][...] = low[:, rows]
    for copy in loads:
        copy.wait()

    hidden_total = w_gate.shape[1]
    hidden_tile, width_tile = tile_of(hidden_total), tile_of(width)
    for number, (first, count) in enumerate(passes):
        rows = count * PAIR_MOST
        wait_blocks(received, recv_sem.at[number], first, count)
        arrived = received[pl.ds(first, count)].astype(F32)
        gathered[:rows, :] = arrived.reshape(rows, width).astype(BF16)

        def expand(tile, carry, rows=rows):
            columns = pl.ds(pl.multiple_of(tile * hidden_tile, hidden_tile), hidden_tile)
            gate_pre = jnp.dot(gathered[:rows, :], w_gate[:, columns], preferred_element_type=F32)
            up_pre = jnp.dot(gathered[:rows, :], w_up[:, columns], preferred_element_type=F32)
            hidden[:rows, columns] = (gate_pre / (1.0 + jnp.exp(-gate_pre)) * up_pre).astype(BF16)
            return carry

        lax.fori_loop(0, hidden_total // hidden_tile, expand, 0, unroll=True)

        def contract(tile, carry, rows=rows, first=first, count=count):
            columns = pl.ds(pl.multiple_of(tile * width_tile, width_tile), width_tile)
            result = jnp.dot(hidden[:rows, :], w_down[:, columns], preferred_element_type=F32)
            produced[pl.ds(first, count), :, columns] = result.reshape(
                count, PAIR_MOST, width_tile
            ).astype(BF16)
            return carry

        lax.fori_loop(0, width // width_tile, contract, 0, unroll=True)
        for entry in results[number]:
            send(produced, back, return_send_sem, return_sem, entry)

    for number, (first, count) in enumerate(groups):
        rows = count * PAIR_MOST
        wait_blocks(back, return_sem.at[number], first, count)
        returned = back[pl.ds(first, count)].astype(F32).reshape(rows, width).astype(BF16)
        result = jnp.dot(mix_hi[number][...], returned, preferred_element_type=F32)
        result += jnp.dot(mix_lo[number][...], returned, preferred_element_type=F32)
        if number:
            result += total[...]
        if number == len(groups) - 1:
            out_ref[...] = result.astype(out_ref.dtype)
        else:
            total[...] = result
    wait_blocks(outgoing, send_sem.at[0], 0, devices - 1)
    wait_blocks(produced, return_send_sem.at[0], 0, devices - 1)


def shards(tokens, w_gate, w_up, w_down, chosen, gate_weights):
    local_count = lax.axis_size("loc")
    devices = lax.axis_size("grp") * local_count
    token_count, width = tokens.shape
    hidden_total = w_gate.shape[2]
    row_total = devices * PAIR_MOST
    block = devices // 4
    pass_rows = (block + max(cuts(block))) * PAIR_MOST
    group_rows = [count * PAIR_MOST for count in group_sizes(block)]
    table = pltpu.VMEM((devices, PAIR_MOST, width), BF16)
    mixes = [pltpu.VMEM((token_count, rows), BF16) for rows in group_rows]
    anywhere = pl.BlockSpec(memory_space=pl.ANY)
    return pl.pallas_call(
        kernel,
        out_shape=pltpu.VMEM((token_count, width), BF16),
        in_specs=[anywhere] * 6,
        out_specs=pl.BlockSpec(memory_space=pltpu.VMEM),
        scratch_shapes=[
            pltpu.VMEM((token_count, width), BF16),
            pltpu.VMEM(w_gate.shape[1:], BF16),
            pltpu.VMEM(w_up.shape[1:], BF16),
            pltpu.VMEM(w_down.shape[1:], BF16),
            pltpu.VMEM(chosen.shape, jnp.int32),
            pltpu.VMEM(chosen.shape, F32),
            pltpu.VMEM((row_total, chosen.shape[1]), jnp.int32),
            pltpu.VMEM((row_total, chosen.shape[1]), F32),
            table,
            table,
            table,
            table,
            pltpu.VMEM((pass_rows, width), BF16),
            pltpu.VMEM((pass_rows, hidden_total), BF16),
            pltpu.VMEM((token_count, width), F32),
            mixes,
            mixes,
            pltpu.SemaphoreType.DMA((3,)),
            pltpu.SemaphoreType.DMA((3 * WEIGHT_CUTS,)),
            pltpu.SemaphoreType.DMA((1,)),
            pltpu.SemaphoreType.DMA((4,)),
            pltpu.SemaphoreType.DMA((1,)),
            pltpu.SemaphoreType.DMA((3,)),
        ],
        compiler_params=pltpu.CompilerParams(
            collective_id=0, has_side_effects=True, vmem_limit_bytes=58 * 1024 * 1024
        ),
    )(tokens, w_gate, w_up, w_down, chosen, gate_weights)


def solution(mesh):
    return jax.shard_map(
        shards,
        mesh=mesh,
        in_specs=(
            P(("grp", "loc"), None),
            P(("grp", "loc"), None, None),
            P(("grp", "loc"), None, None),
            P(("grp", "loc"), None, None),
            P(),
            P(),
        ),
        out_specs=P(("grp", "loc"), None),
        check_vma=False,
    )
```

```python
import jax
import jax.numpy as jnp
from jax import lax
from jax.experimental import pallas as pl
from jax.experimental.pallas import tpu as pltpu
from jax.sharding import PartitionSpec as P

PAIR_MOST = 8
WIDE = 256
WEIGHT_CUTS = 4
MESH = pl.DeviceIdType.MESH
F32 = jnp.float32
BF16 = jnp.bfloat16


def tile_of(size):
    for tile in (WIDE, 128):
        if size % tile == 0:
            return tile
    return size


def cuts(block):
    early = block * 3 // 8
    return early, block - early


def group_sizes(block):
    early, late = cuts(block)
    return [2 * block, 2 * early, 2 * late]


def flip(value, mask):
    bit = 1
    while bit <= mask:
        if mask & bit:
            value = value + bit - 2 * bit * (value // bit % 2)
        bit *= 2
    return value


def kernel(
    tokens_hbm,
    gate_hbm,
    up_hbm,
    down_hbm,
    chosen_hbm,
    weight_hbm,
    out_ref,
    tokens,
    w_gate,
    w_up,
    w_down,
    chosen,
    weights,
    chosen_rows,
    weight_rows,
    outgoing,
    received,
    produced,
    back,
    gathered,
    hidden,
    total,
    mix,
    small_sem,
    load_sem,
    send_sem,
    recv_sem,
    return_send_sem,
    return_sem,
    entered,
):
    group_count, local_count = lax.axis_size("grp"), lax.axis_size("loc")
    devices = group_count * local_count
    quarter = local_count // 4
    grp, loc = lax.axis_index("grp"), lax.axis_index("loc")
    me = grp * local_count + loc
    plane, spot = loc // quarter, loc % quarter
    side = plane // 2
    outer = (side + plane % 2 + 1) % 2
    block = quarter * group_count
    early, late = cuts(block)

    def partner(plane_there, turn):
        return (
            flip(grp, turn % group_count),
            plane_there * quarter + flip(spot, turn // group_count),
        )

    def far_plane(kind):
        return side * (1 - kind) + (1 - side) * (2 + kind)

    def near_out(other, turn):
        return other * block + turn

    def far_out(sub, kind, turn):
        if sub:
            return 2 * block + 2 * early + kind * late + turn
        return 2 * block + kind * early + turn

    def near_in(other, turn):
        return other * (block + early) + turn

    def far_in(sub, kind, turn):
        if sub:
            return 2 * (block + early) + (1 - kind) * late + turn
        return block + kind * (block + early) + turn

    def far_pass(sub, kind):
        return 3 - kind if sub else kind

    far, results = {}, [[], [], [], []]
    for sub, count in enumerate((early, late)):
        for turn in range(count):
            for kind in range(2):
                peer = partner(far_plane(kind), sub * early + turn)
                there, number = far_in(sub, outer, turn), far_pass(sub, outer)
                entry = (far_out(sub, kind, turn), peer, there, number)
                far.setdefault((sub, kind), []).append(entry)
                home = far_out(sub, outer, turn)
                results[far_pass(sub, kind)].append((far_in(sub, kind, turn), peer, home, 1 + sub))
    near = [[], []]
    for other in (1, 0):
        for turn in range(block):
            peer = partner(flip(plane, other), turn)
            near[other].append((near_out(other, turn), peer, near_in(other, turn), other))
            results[other].append((near_in(other, turn), peer, near_out(other, turn), 0))
    mixed = [entry for sub in range(2) for pair in zip(far[sub, 0], far[sub, 1]) for entry in pair]
    dispatch = near[1] + near[0] + mixed
    counts = [block + early, block + early, late, late]
    passes = [(sum(counts[:number]), count) for number, count in enumerate(counts)]
    counts = group_sizes(block)
    groups = [(sum(counts[:number]), count) for number, count in enumerate(counts)]
    barrier = pltpu.get_barrier_semaphore()

    def signal(semaphore, peer):
        pl.semaphore_signal(semaphore, inc=1, device_id=peer, device_id_type=MESH)

    @pl.when(plane != 3)
    def _():
        for _, peer, _, _ in reversed(near[1]):
            signal(barrier, peer)

    for _, peer, _, _ in reversed(near[0][1:] + mixed):
        signal(barrier, peer)
    small = [
        pltpu.make_async_copy(chosen_hbm, chosen, small_sem.at[0]),
        pltpu.make_async_copy(weight_hbm, weights, small_sem.at[1]),
        pltpu.make_async_copy(tokens_hbm, tokens, small_sem.at[2]),
    ]
    for copy in small:
        copy.start()

    small[0].wait()
    small[1].wait()
    slot_total = chosen.shape[1]
    for at, (peer_grp, peer_loc), _, _ in dispatch:
        expert = peer_grp * local_count + peer_loc
        rows = pl.ds(at * PAIR_MOST, PAIR_MOST)
        chosen_rows[rows, :] = jnp.broadcast_to(
            chosen[pl.ds(expert, 1), :], (PAIR_MOST, slot_total)
        )
        weight_rows[rows, :] = jnp.broadcast_to(
            weights[pl.ds(expert, 1), :], (PAIR_MOST, slot_total)
        )
    token_count, width = tokens.shape
    row_total = devices * PAIR_MOST
    local = chosen_rows[...] - me * token_count
    mine = (local >= 0) & (local < token_count)
    earlier = lax.broadcasted_iota(jnp.int32, (slot_total, slot_total), 0)
    later = lax.broadcasted_iota(jnp.int32, (slot_total, slot_total), 1)
    before = jnp.where(earlier < later, 1.0, 0.0).astype(BF16)
    rank = jnp.dot(
        jnp.where(mine, 1.0, 0.0).astype(BF16), before, preferred_element_type=F32
    )
    wanted = lax.broadcasted_iota(jnp.int32, (row_total, slot_total), 0) % PAIR_MOST
    hit = mine & (rank == wanted.astype(F32))
    pick = jnp.sum(jnp.where(hit, local.astype(F32) + 1.0, 0.0), axis=1, keepdims=True) - 1.0
    pick_weight = jnp.sum(jnp.where(hit, weight_rows[...], 0.0), axis=1, keepdims=True)
    token_iota = lax.broadcasted_iota(jnp.int32, (row_total, token_count), 1).astype(F32)
    select = pick == token_iota
    select_table = jnp.where(select, 1.0, 0.0).astype(BF16)
    small[2].wait()
    loads = []
    for number, (source, place) in enumerate(
        ((gate_hbm, w_gate), (up_hbm, w_up), (down_hbm, w_down))
    ):
        depth = place.shape[0] // WEIGHT_CUTS
        for cut in range(WEIGHT_CUTS):
            rows = pl.ds(cut * depth, depth)
            copy = pltpu.make_async_copy(
                source.at[0, rows], place.at[rows], load_sem.at[number * WEIGHT_CUTS + cut]
            )
            copy.start()
            loads.append(copy)
    picked = jnp.dot(select_table, tokens[...], preferred_element_type=F32)
    outgoing[...] = picked.reshape(devices, PAIR_MOST, width).astype(BF16)
    pl.semaphore_wait(barrier, devices - 1 - block * (plane // 2 * (3 - plane)))

    @pl.when(plane == 3)
    def _():
        for _, peer, _, _ in near[1]:
            signal(entered, peer)

    def send(source, place, send_sems, sems, entry):
        at, peer, mirror, sem = entry
        if at:
            pltpu.make_async_remote_copy(
                src_ref=source.at[at],
                dst_ref=place.at[mirror],
                send_sem=send_sems.at[0],
                recv_sem=sems.at[sem],
                device_id=peer,
                device_id_type=MESH,
            ).start()
        else:
            pltpu.make_async_copy(source.at[at], place.at[mirror], sems.at[sem]).start()

    def wait_blocks(place, sem, first, count):
        view = place.at[pl.ds(first, count)]
        pltpu.make_async_copy(view, view, sem).wait()

    @pl.when(plane == 2)
    def _():
        for entry in mixed + near[0]:
            send(outgoing, received, send_sem, recv_sem, entry)
        pl.semaphore_wait(entered, block)
        for entry in near[1]:
            send(outgoing, received, send_sem, recv_sem, entry)

    @pl.when(plane != 2)
    def _():
        for entry in dispatch:
            send(outgoing, received, send_sem, recv_sem, entry)
    mixing = jnp.where(select, pick_weight, 0.0).T
    high = mixing.astype(BF16)
    low = (mixing - high.astype(F32)).astype(BF16)
    for number, (first, count) in enumerate(groups):
        rows = slice(first * PAIR_MOST, (first + count) * PAIR_MOST)
        mix[number][...] = jnp.concatenate([high[:, rows], low[:, rows]], axis=1)
    for copy in loads[: 2 * WEIGHT_CUTS]:
        copy.wait()

    hidden_total = w_gate.shape[1]
    hidden_tile, width_tile = tile_of(hidden_total), tile_of(width)
    for number, (first, count) in enumerate(passes):
        rows = count * PAIR_MOST
        wait_blocks(received, recv_sem.at[number], first, count)
        arrived = received[pl.ds(first, count)].astype(F32)
        gathered[:rows, :] = arrived.reshape(rows, width).astype(BF16)

        def expand(tile, carry, rows=rows):
            columns = pl.ds(pl.multiple_of(tile * hidden_tile, hidden_tile), hidden_tile)
            gate_pre = jnp.dot(gathered[:rows, :], w_gate[:, columns], preferred_element_type=F32)
            up_pre = jnp.dot(gathered[:rows, :], w_up[:, columns], preferred_element_type=F32)
            hidden[:rows, columns] = (gate_pre / (1.0 + jnp.exp(-gate_pre)) * up_pre).astype(BF16)
            return carry

        lax.fori_loop(0, hidden_total // hidden_tile, expand, 0, unroll=True)
        if not number:
            for copy in loads[2 * WEIGHT_CUTS :]:
                copy.wait()

        def contract(tile, carry, rows=rows, first=first, count=count):
            columns = pl.ds(pl.multiple_of(tile * width_tile, width_tile), width_tile)
            result = jnp.dot(hidden[:rows, :], w_down[:, columns], preferred_element_type=F32)
            produced[pl.ds(first, count), :, columns] = result.reshape(
                count, PAIR_MOST, width_tile
            ).astype(BF16)
            return carry

        lax.fori_loop(0, width // width_tile, contract, 0, unroll=True)
        if number < 2:

            @pl.when(side == 1 - number)
            def _():
                for entry in results[0]:
                    send(produced, back, return_send_sem, return_sem, entry)

        if number == 3:
            high = grp // (group_count // 2)
            middle = late * 3 // 5

            @pl.when(high == 0)
            def _():
                for entry in results[3]:
                    send(produced, back, return_send_sem, return_sem, entry)

            @pl.when(high == 1)
            def _():
                for entry in results[3][middle:] + results[3][:middle]:
                    send(produced, back, return_send_sem, return_sem, entry)
        elif number:
            for entry in results[number]:
                send(produced, back, return_send_sem, return_sem, entry)

    for number, (first, count) in enumerate(groups):
        rows = count * PAIR_MOST
        wait_blocks(back, return_sem.at[number], first, count)
        returned = back[pl.ds(first, count)].astype(F32).reshape(rows, width).astype(BF16)
        twice = jnp.concatenate([returned, returned], axis=0)
        result = jnp.dot(mix[number][...], twice, preferred_element_type=F32)
        if number:
            result += total[...]
        if number == len(groups) - 1:
            out_ref[...] = result.astype(out_ref.dtype)
        else:
            total[...] = result
    wait_blocks(outgoing, send_sem.at[0], 0, devices - 1)
    wait_blocks(produced, return_send_sem.at[0], 0, devices - 1)


def shards(tokens, w_gate, w_up, w_down, chosen, gate_weights):
    local_count = lax.axis_size("loc")
    devices = lax.axis_size("grp") * local_count
    token_count, width = tokens.shape
    hidden_total = w_gate.shape[2]
    row_total = devices * PAIR_MOST
    block = devices // 4
    pass_rows = (block + max(cuts(block))) * PAIR_MOST
    group_rows = [count * PAIR_MOST for count in group_sizes(block)]
    table = pltpu.VMEM((devices, PAIR_MOST, width), BF16)
    mixes = [pltpu.VMEM((token_count, 2 * rows), BF16) for rows in group_rows]
    anywhere = pl.BlockSpec(memory_space=pl.ANY)
    return pl.pallas_call(
        kernel,
        out_shape=pltpu.VMEM((token_count, width), BF16),
        in_specs=[anywhere] * 6,
        out_specs=pl.BlockSpec(memory_space=pltpu.VMEM),
        scratch_shapes=[
            pltpu.VMEM((token_count, width), BF16),
            pltpu.VMEM(w_gate.shape[1:], BF16),
            pltpu.VMEM(w_up.shape[1:], BF16),
            pltpu.VMEM(w_down.shape[1:], BF16),
            pltpu.VMEM(chosen.shape, jnp.int32),
            pltpu.VMEM(chosen.shape, F32),
            pltpu.VMEM((row_total, chosen.shape[1]), jnp.int32),
            pltpu.VMEM((row_total, chosen.shape[1]), F32),
            table,
            table,
            table,
            table,
            pltpu.VMEM((pass_rows, width), BF16),
            pltpu.VMEM((pass_rows, hidden_total), BF16),
            pltpu.VMEM((token_count, width), F32),
            mixes,
            pltpu.SemaphoreType.DMA((3,)),
            pltpu.SemaphoreType.DMA((3 * WEIGHT_CUTS,)),
            pltpu.SemaphoreType.DMA((1,)),
            pltpu.SemaphoreType.DMA((4,)),
            pltpu.SemaphoreType.DMA((1,)),
            pltpu.SemaphoreType.DMA((3,)),
            pltpu.SemaphoreType.REGULAR,
        ],
        compiler_params=pltpu.CompilerParams(
            collective_id=0, has_side_effects=True, vmem_limit_bytes=58 * 1024 * 1024
        ),
    )(tokens, w_gate, w_up, w_down, chosen, gate_weights)


def solution(mesh):
    return jax.shard_map(
        shards,
        mesh=mesh,
        in_specs=(
            P(("grp", "loc"), None),
            P(("grp", "loc"), None, None),
            P(("grp", "loc"), None, None),
            P(("grp", "loc"), None, None),
            P(),
            P(),
        ),
        out_specs=P(("grp", "loc"), None),
        check_vma=False,
    )
```

```python
import jax
import jax.numpy as jnp
from jax import lax
from jax.experimental import pallas as pl
from jax.experimental.pallas import tpu as pltpu
from jax.sharding import PartitionSpec as P

PAIR_MOST = 8
WIDE = 256
WEIGHT_CUTS = 4
MESH = pl.DeviceIdType.MESH
F32 = jnp.float32
BF16 = jnp.bfloat16


def tile_of(size):
    for tile in (WIDE, 128):
        if size % tile == 0:
            return tile
    return size


def cuts(block):
    early = block * 3 // 8
    return early, block - early


def group_sizes(block):
    early, late = cuts(block)
    return [2 * block, 2 * early, 2 * late]


def flip(value, mask):
    bit = 1
    while bit <= mask:
        if mask & bit:
            value = value + bit - 2 * bit * (value // bit % 2)
        bit *= 2
    return value


def kernel(
    tokens_hbm,
    gate_hbm,
    up_hbm,
    down_hbm,
    chosen_hbm,
    weight_hbm,
    out_ref,
    tokens,
    w_gate,
    w_up,
    w_down,
    chosen,
    weights,
    chosen_rows,
    weight_rows,
    outgoing,
    received,
    produced,
    back,
    gathered,
    hidden,
    total,
    mix,
    small_sem,
    load_sem,
    send_sem,
    recv_sem,
    return_send_sem,
    return_sem,
    entered,
):
    group_count, local_count = lax.axis_size("grp"), lax.axis_size("loc")
    devices = group_count * local_count
    quarter = local_count // 4
    grp, loc = lax.axis_index("grp"), lax.axis_index("loc")
    me = grp * local_count + loc
    plane, spot = loc // quarter, loc % quarter
    side = plane // 2
    outer = (side + plane % 2 + 1) % 2
    block = quarter * group_count
    early, late = cuts(block)

    def partner(plane_there, turn):
        return (
            flip(grp, turn % group_count),
            plane_there * quarter + flip(spot, turn // group_count),
        )

    def far_plane(kind):
        return side * (1 - kind) + (1 - side) * (2 + kind)

    def near_out(other, turn):
        return other * block + turn

    def far_out(sub, kind, turn):
        if sub:
            return 2 * block + 2 * early + kind * late + turn
        return 2 * block + kind * early + turn

    def near_in(other, turn):
        return other * (block + early) + turn

    def far_in(sub, kind, turn):
        if sub:
            return 2 * (block + early) + (1 - kind) * late + turn
        return block + kind * (block + early) + turn

    def far_pass(sub, kind):
        return 3 - kind if sub else kind

    far, results = {}, [[], [], [], []]
    for sub, count in enumerate((early, late)):
        for turn in range(count):
            for kind in range(2):
                peer = partner(far_plane(kind), sub * early + turn)
                there, number = far_in(sub, outer, turn), far_pass(sub, outer)
                entry = (far_out(sub, kind, turn), peer, there, number)
                far.setdefault((sub, kind), []).append(entry)
                home = far_out(sub, outer, turn)
                results[far_pass(sub, kind)].append((far_in(sub, kind, turn), peer, home, 1 + sub))
    near = [[], []]
    for other in (1, 0):
        for turn in range(block):
            peer = partner(flip(plane, other), turn)
            near[other].append((near_out(other, turn), peer, near_in(other, turn), other))
            results[other].append((near_in(other, turn), peer, near_out(other, turn), 0))
    mixed = [entry for sub in range(2) for pair in zip(far[sub, 0], far[sub, 1]) for entry in pair]
    dispatch = near[1] + near[0] + mixed
    counts = [block + early, block + early, late, late]
    passes = [(sum(counts[:number]), count) for number, count in enumerate(counts)]
    counts = group_sizes(block)
    groups = [(sum(counts[:number]), count) for number, count in enumerate(counts)]
    barrier = pltpu.get_barrier_semaphore()

    def signal(semaphore, peer):
        pl.semaphore_signal(semaphore, inc=1, device_id=peer, device_id_type=MESH)

    @pl.when(plane != 3)
    def _():
        for _, peer, _, _ in reversed(near[1]):
            signal(barrier, peer)

    for _, peer, _, _ in reversed(near[0][1:] + mixed):
        signal(barrier, peer)
    small = [
        pltpu.make_async_copy(chosen_hbm, chosen, small_sem.at[0]),
        pltpu.make_async_copy(weight_hbm, weights, small_sem.at[1]),
        pltpu.make_async_copy(tokens_hbm, tokens, small_sem.at[2]),
    ]
    for copy in small:
        copy.start()

    small[0].wait()
    small[1].wait()
    slot_total = chosen.shape[1]
    for at, (peer_grp, peer_loc), _, _ in dispatch:
        expert = peer_grp * local_count + peer_loc
        rows = pl.ds(at * PAIR_MOST, PAIR_MOST)
        chosen_rows[rows, :] = jnp.broadcast_to(
            chosen[pl.ds(expert, 1), :], (PAIR_MOST, slot_total)
        )
        weight_rows[rows, :] = jnp.broadcast_to(
            weights[pl.ds(expert, 1), :], (PAIR_MOST, slot_total)
        )
    token_count, width = tokens.shape
    row_total = devices * PAIR_MOST
    local = chosen_rows[...] - me * token_count
    mine = (local >= 0) & (local < token_count)
    earlier = lax.broadcasted_iota(jnp.int32, (slot_total, slot_total), 0)
    later = lax.broadcasted_iota(jnp.int32, (slot_total, slot_total), 1)
    before = jnp.where(earlier < later, 1.0, 0.0).astype(BF16)
    rank = jnp.dot(
        jnp.where(mine, 1.0, 0.0).astype(BF16), before, preferred_element_type=F32
    )
    wanted = lax.broadcasted_iota(jnp.int32, (row_total, slot_total), 0) % PAIR_MOST
    hit = mine & (rank == wanted.astype(F32))
    pick = jnp.sum(jnp.where(hit, local.astype(F32) + 1.0, 0.0), axis=1, keepdims=True) - 1.0
    pick_weight = jnp.sum(jnp.where(hit, weight_rows[...], 0.0), axis=1, keepdims=True)
    token_iota = lax.broadcasted_iota(jnp.int32, (row_total, token_count), 1).astype(F32)
    select = pick == token_iota
    select_table = jnp.where(select, 1.0, 0.0).astype(BF16)
    small[2].wait()
    loads = []
    for number, (source, place) in enumerate(
        ((gate_hbm, w_gate), (up_hbm, w_up), (down_hbm, w_down))
    ):
        depth = place.shape[0] // WEIGHT_CUTS
        for cut in range(WEIGHT_CUTS):
            rows = pl.ds(cut * depth, depth)
            copy = pltpu.make_async_copy(
                source.at[0, rows], place.at[rows], load_sem.at[number * WEIGHT_CUTS + cut]
            )
            copy.start()
            loads.append(copy)
    picked = jnp.dot(select_table, tokens[...], preferred_element_type=F32)
    outgoing[...] = picked.reshape(devices, PAIR_MOST, width).astype(BF16)
    pl.semaphore_wait(barrier, devices - 1 - block * (plane // 2 * (3 - plane)))

    @pl.when(plane == 3)
    def _():
        for _, peer, _, _ in near[1]:
            signal(entered, peer)

    def send(source, place, send_sems, sems, entry):
        at, peer, mirror, sem = entry
        if at:
            pltpu.make_async_remote_copy(
                src_ref=source.at[at],
                dst_ref=place.at[mirror],
                send_sem=send_sems.at[0],
                recv_sem=sems.at[sem],
                device_id=peer,
                device_id_type=MESH,
            ).start()
        else:
            pltpu.make_async_copy(source.at[at], place.at[mirror], sems.at[sem]).start()

    def wait_blocks(place, sem, first, count):
        view = place.at[pl.ds(first, count)]
        pltpu.make_async_copy(view, view, sem).wait()

    @pl.when(plane == 2)
    def _():
        for entry in mixed + near[0]:
            send(outgoing, received, send_sem, recv_sem, entry)
        pl.semaphore_wait(entered, block)
        for entry in near[1]:
            send(outgoing, received, send_sem, recv_sem, entry)

    @pl.when(plane != 2)
    def _():
        for entry in dispatch:
            send(outgoing, received, send_sem, recv_sem, entry)
    mixing = jnp.where(select, pick_weight, 0.0).T
    high = mixing.astype(BF16)
    low = (mixing - high.astype(F32)).astype(BF16)
    for number, (first, count) in enumerate(groups):
        rows = slice(first * PAIR_MOST, (first + count) * PAIR_MOST)
        mix[number][...] = jnp.concatenate([high[:, rows], low[:, rows]], axis=1)
    filled = passes[0][1] * PAIR_MOST
    if filled < gathered.shape[0]:
        gathered[filled:, :] = jnp.zeros_like(gathered[filled:, :])
    for copy in loads[: 2 * WEIGHT_CUTS]:
        copy.wait()

    hidden_total = w_gate.shape[1]
    hidden_tile, width_tile = tile_of(hidden_total), tile_of(width)
    full = gathered.shape[0]
    for number, (first, count) in enumerate(passes):
        rows = count * PAIR_MOST
        wait_blocks(received, recv_sem.at[number], first, count)
        arrived = received[pl.ds(first, count)].astype(F32)
        gathered[:rows, :] = arrived.reshape(rows, width).astype(BF16)

        def expand(tile, carry):
            columns = pl.ds(pl.multiple_of(tile * hidden_tile, hidden_tile), hidden_tile)
            gate_pre = jnp.dot(gathered[:full, :], w_gate[:, columns], preferred_element_type=F32)
            up_pre = jnp.dot(gathered[:full, :], w_up[:, columns], preferred_element_type=F32)
            hidden[:full, columns] = (gate_pre / (1.0 + jnp.exp(-gate_pre)) * up_pre).astype(BF16)
            return carry

        lax.fori_loop(0, hidden_total // hidden_tile, expand, 0, unroll=True)
        if not number:
            for copy in loads[2 * WEIGHT_CUTS :]:
                copy.wait()

        def contract(tile, carry, rows=rows, first=first, count=count):
            columns = pl.ds(pl.multiple_of(tile * width_tile, width_tile), width_tile)
            result = jnp.dot(hidden[:full, :], w_down[:, columns], preferred_element_type=F32)
            produced[pl.ds(first, count), :, columns] = result[:rows].reshape(
                count, PAIR_MOST, width_tile
            ).astype(BF16)
            return carry

        lax.fori_loop(0, width // width_tile, contract, 0, unroll=True)
        if number < 2:

            @pl.when(side == 1 - number)
            def _():
                for entry in results[0]:
                    send(produced, back, return_send_sem, return_sem, entry)

        if number == 3:
            high = grp // (group_count // 2)
            middle = late * 3 // 5

            @pl.when(high == 0)
            def _():
                for entry in results[3]:
                    send(produced, back, return_send_sem, return_sem, entry)

            @pl.when(high == 1)
            def _():
                for entry in results[3][middle:] + results[3][:middle]:
                    send(produced, back, return_send_sem, return_sem, entry)
        elif number:
            for entry in results[number]:
                send(produced, back, return_send_sem, return_sem, entry)

    for number, (first, count) in enumerate(groups):
        rows = count * PAIR_MOST
        wait_blocks(back, return_sem.at[number], first, count)
        returned = back[pl.ds(first, count)].astype(F32).reshape(rows, width).astype(BF16)
        twice = jnp.concatenate([returned, returned], axis=0)
        result = jnp.dot(mix[number][...], twice, preferred_element_type=F32)
        if number:
            result += total[...]
        if number == len(groups) - 1:
            out_ref[...] = result.astype(out_ref.dtype)
        else:
            total[...] = result
    wait_blocks(outgoing, send_sem.at[0], 0, devices - 1)
    wait_blocks(produced, return_send_sem.at[0], 0, devices - 1)


def shards(tokens, w_gate, w_up, w_down, chosen, gate_weights):
    local_count = lax.axis_size("loc")
    devices = lax.axis_size("grp") * local_count
    token_count, width = tokens.shape
    hidden_total = w_gate.shape[2]
    row_total = devices * PAIR_MOST
    block = devices // 4
    pass_rows = -(-(block + max(cuts(block))) * PAIR_MOST // 32) * 32
    group_rows = [count * PAIR_MOST for count in group_sizes(block)]
    table = pltpu.VMEM((devices, PAIR_MOST, width), BF16)
    mixes = [pltpu.VMEM((token_count, 2 * rows), BF16) for rows in group_rows]
    anywhere = pl.BlockSpec(memory_space=pl.ANY)
    return pl.pallas_call(
        kernel,
        out_shape=pltpu.VMEM((token_count, width), BF16),
        in_specs=[anywhere] * 6,
        out_specs=pl.BlockSpec(memory_space=pltpu.VMEM),
        scratch_shapes=[
            pltpu.VMEM((token_count, width), BF16),
            pltpu.VMEM(w_gate.shape[1:], BF16),
            pltpu.VMEM(w_up.shape[1:], BF16),
            pltpu.VMEM(w_down.shape[1:], BF16),
            pltpu.VMEM(chosen.shape, jnp.int32),
            pltpu.VMEM(chosen.shape, F32),
            pltpu.VMEM((row_total, chosen.shape[1]), jnp.int32),
            pltpu.VMEM((row_total, chosen.shape[1]), F32),
            table,
            table,
            table,
            table,
            pltpu.VMEM((pass_rows, width), BF16),
            pltpu.VMEM((pass_rows, hidden_total), BF16),
            pltpu.VMEM((token_count, width), F32),
            mixes,
            pltpu.SemaphoreType.DMA((3,)),
            pltpu.SemaphoreType.DMA((3 * WEIGHT_CUTS,)),
            pltpu.SemaphoreType.DMA((1,)),
            pltpu.SemaphoreType.DMA((4,)),
            pltpu.SemaphoreType.DMA((1,)),
            pltpu.SemaphoreType.DMA((3,)),
            pltpu.SemaphoreType.REGULAR,
        ],
        compiler_params=pltpu.CompilerParams(
            collective_id=0, has_side_effects=True, vmem_limit_bytes=58 * 1024 * 1024
        ),
    )(tokens, w_gate, w_up, w_down, chosen, gate_weights)


def solution(mesh):
    return jax.shard_map(
        shards,
        mesh=mesh,
        in_specs=(
            P(("grp", "loc"), None),
            P(("grp", "loc"), None, None),
            P(("grp", "loc"), None, None),
            P(("grp", "loc"), None, None),
            P(),
            P(),
        ),
        out_specs=P(("grp", "loc"), None),
        check_vma=False,
    )
```
